256 devices in a mesh: ctx: 64 (over x, z, core), head: 4 (over y).
Axes of the slice: x: 4, y: 4, z: 8, core: 2. Of those that a mesh axis runs over, the one named last changes fastest.
Arguments:
- query: bfloat16 [49152, 1024], P('ctx', 'head'), parts along dimension 1, may hold values from -6 to 6
- key_value: bfloat16 [49152, 1024], P('ctx', 'head'), parts along dimension 1, may hold values from -6 to 6
- d_out: bfloat16 [49152, 1024], P('ctx', 'head'), parts along dimension 1, may hold values from -128 to 128
- doc_starts: int32 [512], P('head'), parts along dimension 0, may hold values from 0 to 49151, as said below
Outputs:
- d_query: bfloat16 [49152, 1024], P('ctx', 'head'), parts along dimension 1
- d_key_value: bfloat16 [49152, 1024], P('ctx', 'head'), parts along dimension 1
The draws below stay inside these ranges and needn't reach their ends.
There are 4 independent parts, one for each index of `head`. The reference program is written for one: setup_inputs(seed, part) draws one part's arguments, and reference() takes and returns one part's arrays. A program takes and returns all parts, laid end to end along the dimension named above; each array names one. Nothing has to cross between parts.
Inputs may be any that keep to these rules, and one draw needn't show every extreme that they name: `doc_starts`: Non-decreasing, first entry 0; the document of position p runs from the largest entry not above p up to the next larger entry or 49152; repeated entries are empty documents. A position p never belongs to a document that begins before (p // 768 - 3) * 768, and in every draw some document begins in the block of 768 positions exactly 3 blocks before the block of its last position.
All inputs are finite; a program needn't handle non-finite values.
Results may differ from the reference program's by a relative error of at most 0.0055.
Values may be sent and summed in bfloat16 or wider, within the bound.
A program may use at most 128 MiB of HBM per device.

```python
import jax
import jax.numpy as jnp
from jax import lax

HD = 128
QH = 2
HOPS = 3
TOK_DEV = 768
TOKENS = 49152
STARTS = 128


def start_list(key):
    base = jax.random.fold_in(key, 7001)
    key_offsets, key_anchor, key_coin, key_long = jax.random.split(base, 4)
    half_block = TOK_DEV // 2
    count = STARTS
    group_size = HOPS
    group_count = (count + group_size - 1) // group_size
    strata = jnp.arange(count, dtype=jnp.int32)
    offsets = jax.random.randint(key_offsets, (count,), 0, half_block, dtype=jnp.int32)
    anchor_pick = jax.random.randint(key_anchor, (group_count,), 0, group_size, dtype=jnp.int32)
    anchors = jnp.minimum(jnp.arange(group_count, dtype=jnp.int32) * group_size + anchor_pick, count - 1)
    is_anchor = anchors[strata // group_size] == strata
    coins = jax.random.randint(key_coin, (count,), 0, 2, dtype=jnp.int32) == 1
    keeping = is_anchor | coins | (strata == 0)
    options = (count // group_size - 1) // 2
    long_group = 2 * jax.random.randint(key_long, (), 0, options, dtype=jnp.int32) + 1
    lower = long_group * group_size
    upper = (long_group + 2) * group_size - 1
    inside = (strata > lower) & (strata < upper)
    keeping = jnp.where(inside, False, keeping) | (strata == lower) | (strata == upper)
    offsets = jnp.where(strata == lower, 0, jnp.where(strata == upper, half_block - 1, offsets))
    offsets = jnp.where(strata == 0, 0, offsets)
    cuts = strata * half_block + offsets
    return lax.cummax(jnp.where(keeping, cuts, 0), axis=0).astype(jnp.int32)


def query_and_pairs(key):
    base = jax.random.fold_in(key, 7002)
    key_query, key_keys, key_values = jax.random.split(base, 3)
    queries = jnp.clip(jax.random.normal(key_query, (TOKENS, QH * HD), jnp.float32), -6.0, 6.0)
    keys_drawn = jnp.clip(jax.random.normal(key_keys, (TOKENS, HD), jnp.float32), -6.0, 6.0)
    values_drawn = jnp.clip(jax.random.normal(key_values, (TOKENS, HD), jnp.float32), -6.0, 6.0)
    return (queries, jnp.concatenate([keys_drawn, values_drawn], axis=1))


def draw_query(key, part):
    return query_and_pairs(key)[0].astype(jnp.bfloat16)


def draw_key_value(key, part):
    return query_and_pairs(key)[1].astype(jnp.bfloat16)


def draw_doc_starts(key, part):
    return start_list(key)


def shard_levels(rng, dims, cuts, low, top_value):
    def one(dim, blocks):
        steps = jax.random.uniform(jax.random.fold_in(jax.random.fold_in(rng, 6), dim), (blocks,), jnp.float32, low / len(cuts), top_value / len(cuts))
        return jnp.repeat(jnp.exp(steps), dims[dim] // blocks).reshape((-1,) + (1,) * (len(dims) - dim - 1))

    factor_of = one(*cuts[0])
    for cut in cuts[1:]:
        factor_of = factor_of * one(*cut)
    return factor_of


def normal_values(stream_key, dims, spread, bound, cuts=(), kind=jnp.bfloat16):
    values = spread * jax.random.normal(stream_key, dims, jnp.float32)
    if cuts:
        values = values * shard_levels(stream_key, dims, cuts, -0.22, 0.18)
    return jnp.clip(values, -bound, bound).astype(kind)


def setup_inputs(seed: int = 0, part: int = 0) -> dict:
    key_of = jax.random.split(jax.random.key(seed), 5)
    part_splits = jax.random.split(jax.random.fold_in(key_of[4], part), 5)
    return {
        "query": draw_query(jax.random.fold_in(jax.random.fold_in(key_of[4], part), 71), part),
        "key_value": draw_key_value(jax.random.fold_in(jax.random.fold_in(key_of[4], part), 71), part),
        "d_out": normal_values(part_splits[2], (TOKENS, QH * HD), 24.0, 128.0, ((0, 64),)),
        "doc_starts": draw_doc_starts(jax.random.fold_in(jax.random.fold_in(key_of[4], part), 71), part),
    }


def start_of(doc_starts, positions):
    earlier = doc_starts[None, :] <= positions[:, None]
    return jnp.max(jnp.where(earlier, doc_starts[None, :], 0), axis=1).astype(jnp.int32)


def reference(query, key_value, d_out, doc_starts):
    score_scale = HD ** -0.5
    reach = HOPS * TOK_DEV
    window = reach + TOK_DEV
    padded = jnp.concatenate([jnp.zeros((reach, 2 * HD), key_value.dtype), key_value], axis=0)

    def block_terms(block_index):
        first_row = (block_index * TOK_DEV).astype(jnp.int32)
        queries = lax.dynamic_slice_in_dim(query, first_row, TOK_DEV, 0).reshape(TOK_DEV, QH, HD).astype(jnp.float32)
        grads_out = lax.dynamic_slice_in_dim(d_out, first_row, TOK_DEV, 0).reshape(TOK_DEV, QH, HD).astype(jnp.float32)
        kv_window = lax.dynamic_slice_in_dim(padded, first_row, window, 0)
        key_block = kv_window[:, :HD].astype(jnp.float32)
        value_block = kv_window[:, HD:].astype(jnp.float32)
        query_pos = first_row + jnp.arange(TOK_DEV, dtype=jnp.int32)
        key_pos = first_row - reach + jnp.arange(window, dtype=jnp.int32)
        owners = start_of(doc_starts, query_pos)
        visible = ((key_pos[None, :] >= owners[:, None]) & (key_pos[None, :] <= query_pos[:, None]))[None]
        scores = jnp.einsum("thd,sd->hts", queries, key_block) * score_scale
        row_top = jnp.max(jnp.where(visible, scores, -jnp.inf), axis=2)
        row_total = jnp.sum(jnp.where(visible, jnp.exp(scores - row_top[:, :, None]), 0.0), axis=2)
        log_total = row_top + jnp.log(row_total)
        weights = jnp.where(visible, jnp.exp(scores - log_total[:, :, None]), 0.0)
        grad_prob = jnp.einsum("thd,sd->hts", grads_out, value_block)
        row_delta = jnp.sum(weights * grad_prob, axis=2)
        grad_score = (weights * (grad_prob - row_delta[:, :, None]) * score_scale).astype(jnp.bfloat16)
        grad_score = lax.optimization_barrier(grad_score).astype(jnp.float32)
        low_weights = lax.optimization_barrier(weights.astype(jnp.bfloat16)).astype(jnp.float32)
        grad_query = jnp.einsum("hts,sd->thd", grad_score, key_block).reshape(TOK_DEV, QH * HD).astype(jnp.bfloat16)
        grad_key = jnp.einsum("hts,thd->sd", grad_score, queries)
        grad_value = jnp.einsum("hts,thd->sd", low_weights, grads_out)
        shares = jnp.concatenate([grad_key, grad_value], axis=1).astype(jnp.bfloat16)
        shares = lax.optimization_barrier(shares).astype(jnp.float32)
        return grad_query, shares

    def advance(carried, block_index):
        grad_query, shares = block_terms(block_index)
        first_row = (block_index * TOK_DEV).astype(jnp.int32)
        current = lax.dynamic_slice_in_dim(carried, first_row, window, 0)
        carried = lax.dynamic_update_slice_in_dim(carried, current + shares, first_row, 0)
        return carried, grad_query

    blocks = TOKENS // TOK_DEV
    initial = jnp.zeros((reach + TOKENS, 2 * HD), jnp.float32)
    carried, grad_queries = lax.scan(advance, initial, jnp.arange(blocks, dtype=jnp.int32))
    return grad_queries.reshape(TOKENS, QH * HD), carried[reach:].astype(jnp.bfloat16)
```

```python
import functools

import jax
import jax.numpy as jnp
from jax import lax
from jax.experimental import pallas as pl
from jax.experimental.pallas import tpu as pltpu
from jax.sharding import PartitionSpec as P

MESH = pl.DeviceIdType.MESH
HOPS = 3
CHUNK = 256
NEG = -1e30
F32 = jnp.float32
BF16 = jnp.bfloat16


def dot(a, b):
    return lax.dot_general(a, b, (((1,), (0,)), ((), ())), preferred_element_type=F32)


def dot_t(a, b):
    return lax.dot_general(a, b, (((1,), (1,)), ((), ())), preferred_element_type=F32)


def kernel(
    n, q_hbm, kv_hbm, g_hbm, starts, dq_out, dkv_out,
    qv, gv, kb, vb, qt, gt, kt, startr, eb, gp, sbuf, mrun, trun, mblk, dblk, scl, dlt, dqt,
    own_v, own_k, shv, shk, rbv, rbk,
    load_sem, sk, sv, rk, rv, sent_v, sent_k, got_v, got_k,
):
    me = lax.axis_index("ctx")
    row = lax.axis_index("head")
    odd = lax.rem(me, 2)
    even = odd == 0
    t, d = kb.shape[1], kb.shape[2]
    heads = qt.shape[0]
    chunks = t // CHUNK
    unit = d ** (-0.5)
    to_exp2 = unit * 1.4426950408889634

    def dev(step):
        return (lax.rem(me + step + n, n), row)

    loads = [
        pltpu.make_async_copy(kv_hbm.at[:, pl.ds(0, d)], kb.at[0], load_sem.at[0]),
        pltpu.make_async_copy(q_hbm, qv, load_sem.at[1]),
        pltpu.make_async_copy(kv_hbm.at[:, pl.ds(d, d)], vb.at[0], load_sem.at[2]),
        pltpu.make_async_copy(g_hbm, gv, load_sem.at[3]),
    ]
    for load in loads:
        load.start()

    barrier = pltpu.get_barrier_semaphore()

    def greet(steps):
        for step in steps:
            pl.semaphore_signal(barrier, inc=1, device_id=dev(step), device_id_type=MESH)
        pl.semaphore_wait(barrier, len(steps))

    @pl.when(even)
    def _():
        greet((1, -1, 2, -2, 3))

    @pl.when(odd == 1)
    def _():
        greet((1, -1, -3))

    def forward(buf, send, recv, which, source, slot, step):
        return pltpu.make_async_remote_copy(
            src_ref=buf.at[source], dst_ref=buf.at[slot],
            send_sem=send.at[which], recv_sem=recv.at[slot],
            device_id=dev(step), device_id_type=MESH,
        )

    def to_link(buf, send, recv):
        return forward(buf, send, recv, 0, 0, 3 - 2 * odd, 3 - 2 * odd)

    def to_partner(buf, send, recv):
        return forward(buf, send, recv, 1, 0, 1, 1)

    def relay_partner(buf, send, recv):
        return forward(buf, send, recv, 2, 1 + 2 * odd, 2, 1 - 2 * odd)

    def relay_link(buf, send, recv):
        return forward(buf, send, recv, 3, 1, 3, 2)

    loads[0].wait()
    to_link(kb, sk, rk).start()

    @pl.when(even)
    def _():
        to_partner(kb, sk, rk).start()

    loads[1].wait()
    for h in range(heads):
        qt[h] = qv[:, h * d:(h + 1) * d].T
    kt[0] = kb[0].T

    positions = me * t + lax.broadcasted_iota(jnp.int32, (1, t), 1)

    def latest(index, best):
        start = starts[index]
        return jnp.maximum(best, jnp.where(start <= positions, start, 0))

    startr[...] = lax.fori_loop(0, starts.shape[0], latest, jnp.zeros((1, t), jnp.int32))

    def scores(b, own):
        for h in range(heads):
            for c in range(chunks):
                lanes = slice(c * CHUNK, (c + 1) * CHUNK)
                rows = (c + 1) * CHUNK if own else t
                slot = (h * chunks + c) % 2
                s = dot(kb[b, :rows, :], qt[h, :, lanes]) * to_exp2
                j = lax.broadcasted_iota(jnp.int32, (rows, CHUNK), 0)
                visible = j >= startr[:, lanes] - (me - b) * t
                if own:
                    p = lax.broadcasted_iota(jnp.int32, (rows, CHUNK), 1) + c * CHUNK
                    visible = visible & (j <= p)
                s = jnp.where(visible, s, NEG)
                sbuf[slot, :rows, :] = s
                top = jnp.max(s, axis=0, keepdims=True)
                if not own:
                    before = mrun[h:h + 1, lanes]
                    top = jnp.maximum(before, top)
                e = jnp.exp2(sbuf[slot, :rows, :] - top)
                total = jnp.sum(e, axis=0, keepdims=True)
                if not own:
                    total = total + trun[h:h + 1, lanes] * jnp.exp2(before - top)
                eb[b, h, :rows, lanes] = e.astype(BF16)
                if rows < t:
                    eb[b, h, rows:, lanes] = jnp.zeros((t - rows, CHUNK), BF16)
                mrun[h:h + 1, lanes] = top
                mblk[b, h:h + 1, lanes] = top
                trun[h:h + 1, lanes] = total

    def grad_probs(b, own):
        for h in range(heads):
            for c in range(chunks):
                lanes = slice(c * CHUNK, (c + 1) * CHUNK)
                rows = (c + 1) * CHUNK if own else t
                x = dot(vb[b, :rows, :], gt[h, :, lanes])
                gp[b, h, :rows, lanes] = x
                dblk[b, h:h + 1, lanes] = jnp.sum(
                    eb[b, h, :rows, lanes].astype(F32) * x, axis=0, keepdims=True
                )

    def grad_scores(b, own):
        for h in range(heads):
            for c in range(chunks):
                lanes = slice(c * CHUNK, (c + 1) * CHUNK)
                rows = (c + 1) * CHUNK if own else t
                eb[b, h, :rows, lanes] = (
                    eb[b, h, :rows, lanes].astype(F32) * (gp[b, h, :rows, lanes] - dlt[h:h + 1, lanes])
                ).astype(BF16)

    def contract(b, rights, factor):
        total = None
        for h in range(heads):
            right = (rights[h].astype(F32) * (scl[b, h:h + 1, :] * factor)).astype(BF16)
            term = dot_t(eb[b, h], right)
            total = term if total is None else total + term
        return total

    def grad_query(b, first):
        for h in range(heads):
            for c in range(chunks):
                lanes = slice(c * CHUNK, (c + 1) * CHUNK)
                x = dot(kt[b], eb[b, h, :, lanes]) * (scl[b, h:h + 1, lanes] * unit)
                dqt[h, :, lanes] = x if first else dqt[h, :, lanes] + x

    scores(0, True)
    loads[2].wait()
    loads[3].wait()
    for h in range(heads):
        gt[h] = gv[:, h * d:(h + 1) * d].T
    grad_probs(0, True)

    def arrive(step):
        return jnp.where(jnp.logical_and(odd == 1, step > 1), 5 - step, step)

    def await_block(buf, send, recv, b):
        forward(buf, send, recv, 0, 0, b, 1).wait_recv()

    def k_step(step, carry):
        b = arrive(step)
        await_block(kb, sk, rk, b)

        @pl.when(jnp.logical_and(even, step == 1))
        def _():
            relay_link(kb, sk, rk).start()
            relay_partner(kb, sk, rk).start()
            to_link(vb, sv, rv).start()
            to_partner(vb, sv, rv).start()

        @pl.when(jnp.logical_and(odd == 1, step == 2))
        def _():
            relay_partner(kb, sk, rk).start()
            to_link(vb, sv, rv).start()

        scores(b, False)
        kt[b] = kb[b].T
        return carry

    lax.fori_loop(1, HOPS + 1, k_step, 0)

    for h in range(heads):
        inverse = 1.0 / trun[h:h + 1, :]
        for b in range(HOPS + 1):
            scl[b, h:h + 1, :] = jnp.exp2(mblk[b, h:h + 1, :] - mrun[h:h + 1, :]) * inverse

    def off_of(step):
        on_odd = jnp.where(step == 2, 3, 2 - step)
        return jnp.where(even, 3 - step, on_odd)

    def back(send_buf, land, send, recv, off):
        step = jnp.where(even, jnp.where(off == 1, -1, jnp.where(off == 2, 1, -2)), jnp.where(off == 3, -3, -1))
        slot = jnp.where(off == 1, 2, jnp.where(off == 2, 0, jnp.where(even, 1, 3)))
        return pltpu.make_async_remote_copy(
            src_ref=send_buf.at[off], dst_ref=land.at[slot],
            send_sem=send.at[off], recv_sem=recv.at[slot],
            device_id=dev(step), device_id_type=MESH,
        )

    def landed(send_buf, land, send, recv, slot):
        pltpu.make_async_remote_copy(
            src_ref=land.at[slot], dst_ref=land.at[slot],
            send_sem=send.at[0], recv_sem=recv.at[slot],
            device_id=dev(1), device_id_type=MESH,
        ).wait_recv()

    sides = {"v": (shv, rbv, sent_v, got_v), "k": (shk, rbk, sent_k, got_k)}

    def share_step(side, rights, factor):
        send_buf, land, send, recv = sides[side]

        def run(step, carry):
            off = off_of(step)
            if side == "k":
                grad_scores(off, False)
            send_buf[off] = contract(off, rights, factor).astype(BF16)

            @pl.when(step < 2)
            def _():
                back(send_buf, land, send, recv, off).start()

            return carry

        lax.fori_loop(0, HOPS, run, 0)

        @pl.when(odd == 1)
        def _():
            landed(*sides[side], 0)
            send_buf[3] = (send_buf[3].astype(F32) + land[0].astype(F32)).astype(BF16)
            back(*sides[side], 3).start()

    def combine_even(side):
        send_buf, land, send, recv = sides[side]

        @pl.when(even)
        def _():
            landed(*sides[side], 0)
            landed(*sides[side], 1)
            send_buf[1] = (
                send_buf[1].astype(F32) + land[0].astype(F32) + land[1].astype(F32)
            ).astype(BF16)
            back(*sides[side], 1).start()

    share_step("v", gt, 1.0)

    def v_step(step, carry):
        b = arrive(step)
        await_block(vb, sv, rv, b)

        @pl.when(jnp.logical_and(even, step == 1))
        def _():
            relay_link(vb, sv, rv).start()
            relay_partner(vb, sv, rv).start()

        @pl.when(jnp.logical_and(odd == 1, step == 2))
        def _():
            relay_partner(vb, sv, rv).start()

        grad_probs(b, False)
        return carry

    lax.fori_loop(1, HOPS + 1, v_step, 0)
    combine_even("v")

    for h in range(heads):
        delta = None
        for b in range(HOPS + 1):
            term = dblk[b, h:h + 1, :] * scl[b, h:h + 1, :]
            delta = term if delta is None else delta + term
        dlt[h:h + 1, :] = delta

    share_step("k", qt, unit)

    own_v[...] = contract(0, gt, 1.0)
    grad_scores(0, True)
    own_k[...] = contract(0, qt, unit)
    combine_even("k")

    grad_query(0, True)

    def dq_step(b, carry):
        grad_query(b, False)
        return carry

    lax.fori_loop(1, HOPS + 1, dq_step, 0)
    for h in range(heads):
        dq_out[:, h * d:(h + 1) * d] = dqt[h].T.astype(BF16)

    for side, own, column in (("v", own_v, d), ("k", own_k, 0)):
        send_buf, land, send, recv = sides[side]
        landed(*sides[side], 2)
        own[...] = own[...] + land[2].astype(F32)

        @pl.when(even)
        def _():
            landed(*sides[side], 3)
            own[...] = own[...] + land[3].astype(F32)

        dkv_out[:, column:column + d] = own[...].astype(BF16)

    for buf, send, recv in ((kb, sk, rk), (vb, sv, rv)):
        to_link(buf, send, recv).wait_send()
        relay_partner(buf, send, recv).wait_send()

        @pl.when(even)
        def _():
            to_partner(buf, send, recv).wait_send()
            relay_link(buf, send, recv).wait_send()

    for side in ("v", "k"):
        for off in range(1, HOPS + 1):
            back(*sides[side], off).wait_send()


def shards(n, query, key_value, d_out, doc_starts):
    t, width = key_value.shape
    d = width // 2
    heads = query.shape[1] // d
    blocks = HOPS + 1
    any_spec = pl.BlockSpec(memory_space=pl.ANY)
    vmem = pltpu.VMEM
    dma = pltpu.SemaphoreType.DMA
    return pl.pallas_call(
        functools.partial(kernel, n),
        out_shape=(
            jax.ShapeDtypeStruct(query.shape, BF16),
            jax.ShapeDtypeStruct(key_value.shape, BF16),
        ),
        in_specs=[any_spec, any_spec, any_spec, pl.BlockSpec(memory_space=pltpu.SMEM)],
        out_specs=(pl.BlockSpec(memory_space=vmem), pl.BlockSpec(memory_space=vmem)),
        scratch_shapes=[
            vmem((t, heads * d), BF16), vmem((t, heads * d), BF16),
            vmem((blocks, t, d), BF16), vmem((blocks, t, d), BF16),
            vmem((heads, d, t), BF16), vmem((heads, d, t), BF16), vmem((blocks, d, t), BF16),
            vmem((1, t), jnp.int32),
            vmem((blocks, heads, t, t), BF16), vmem((blocks, heads, t, t), F32),
            vmem((2, t, CHUNK), F32),
            vmem((heads, t), F32), vmem((heads, t), F32),
            vmem((blocks, heads, t), F32), vmem((blocks, heads, t), F32), vmem((blocks, heads, t), F32),
            vmem((heads, t), F32), vmem((heads, d, t), F32),
            vmem((t, d), F32), vmem((t, d), F32),
            vmem((blocks, t, d), BF16), vmem((blocks, t, d), BF16),
            vmem((blocks, t, d), BF16), vmem((blocks, t, d), BF16),
            dma((4,)), dma((4,)), dma((4,)), dma((4,)), dma((4,)),
            dma((4,)), dma((4,)), dma((4,)), dma((4,)),
        ],
        compiler_params=pltpu.CompilerParams(
            collective_id=0, has_side_effects=True, vmem_limit_bytes=60 * 1024 * 1024
        ),
    )(query, key_value, d_out, doc_starts)


def solution(mesh):
    placed = (P("ctx", "head"), P("ctx", "head"), P("ctx", "head"), P("head"))
    return jax.shard_map(
        functools.partial(shards, mesh.shape["ctx"]),
        mesh=mesh,
        in_specs=placed,
        out_specs=(P("ctx", "head"), P("ctx", "head")),
        check_vma=False,
    )
```

```python
import functools

import jax
import jax.numpy as jnp
from jax import lax
from jax.experimental import pallas as pl
from jax.experimental.pallas import tpu as pltpu
from jax.sharding import PartitionSpec as P

MESH = pl.DeviceIdType.MESH
HOPS = 3
CHUNK = 256
PIECES = 3
NEG = -1e30
F32 = jnp.float32
BF16 = jnp.bfloat16


def dot(a, b):
    return lax.dot_general(a, b, (((1,), (0,)), ((), ())), preferred_element_type=F32)


def dot_t(a, b):
    return lax.dot_general(a, b, (((1,), (1,)), ((), ())), preferred_element_type=F32)


def kernel(
    n, q_hbm, kv_hbm, g_hbm, starts_hbm, dq_out, dkv_out,
    starts, qv, gv, kb, vb, qt, gt, kt, startr, eb, gp, sbuf, mrun, trun, mblk, dblk, scl, dlt, dqt,
    own_v, own_k, shv, shk, rbv, rbk,
    load_sem, sk, sv, rk, rv, sent_v, sent_k, got_v, got_k,
):
    me = lax.axis_index("ctx")
    row = lax.axis_index("head")
    odd = lax.rem(me, 2)
    even = odd == 0
    t, d = kb.shape[1], kb.shape[2]
    heads = qt.shape[0]
    chunks = t // CHUNK
    unit = d ** (-0.5)
    to_exp2 = unit * 1.4426950408889634

    def dev(step):
        return (lax.rem(me + step + n, n), row)

    loads = [
        pltpu.make_async_copy(kv_hbm.at[:, pl.ds(0, d)], kb.at[0], load_sem.at[0]),
        pltpu.make_async_copy(q_hbm, qv, load_sem.at[1]),
        pltpu.make_async_copy(kv_hbm.at[:, pl.ds(d, d)], vb.at[0], load_sem.at[2]),
        pltpu.make_async_copy(g_hbm, gv, load_sem.at[3]),
        pltpu.make_async_copy(starts_hbm, starts, load_sem.at[4]),
    ]
    for load in loads:
        load.start()

    barrier = pltpu.get_barrier_semaphore()

    def greet(steps):
        for step in steps:
            pl.semaphore_signal(barrier, inc=1, device_id=dev(step), device_id_type=MESH)
        pl.semaphore_wait(barrier, len(steps))

    @pl.when(even)
    def _():
        greet((1, -1, 2, -2, 3))

    @pl.when(odd == 1)
    def _():
        greet((1, -1, -3))

    piece = t // PIECES
    keys = (kb, sk, rk)
    values = (vb, sv, rv)

    def forward(group, which, source, slot, step, r):
        buf, send, recv = group
        rows = pl.ds(r * piece, piece)
        return pltpu.make_async_remote_copy(
            src_ref=buf.at[source, rows], dst_ref=buf.at[slot, rows],
            send_sem=send.at[which, r], recv_sem=recv.at[slot, r],
            device_id=dev(step), device_id_type=MESH,
        )

    def to_link(group, r):
        return forward(group, 0, 0, 3 - 2 * odd, 3 - 2 * odd, r)

    def to_partner(group, r):
        return forward(group, 1, 0, 1, 1, r)

    def relay_partner(group, r):
        return forward(group, 2, 1 + 2 * odd, 2, 1 - 2 * odd, r)

    def relay_link(group, r):
        return forward(group, 3, 1, 3, 2, r)

    def await_piece(group, slot, r):
        forward(group, 0, 0, slot, 1, r).wait_recv()

    def await_block(group, slot):
        for r in range(PIECES):
            await_piece(group, slot, r)

    def send_own_link(group):
        for r in range(PIECES):
            to_link(group, r).start()

    def send_own_partner(group):
        for r in range(PIECES):
            to_partner(group, r).start()

    def pass_on_even(group, r):
        await_piece(group, 1, r)
        relay_link(group, r).start()
        relay_partner(group, r).start()

    def pass_on_odd(group, r):
        await_piece(group, 3, r)
        relay_partner(group, r).start()

    loads[0].wait()
    send_own_link(keys)

    @pl.when(even)
    def _():
        send_own_partner(keys)

    loads[1].wait()
    loads[4].wait()
    for h in range(heads):
        qt[h] = qv[:, h * d:(h + 1) * d].T
    kt[0] = kb[0].T

    positions = me * t + lax.broadcasted_iota(jnp.int32, (1, t), 1)

    def latest(index, best):
        start = starts[index]
        return jnp.maximum(best, jnp.where(start <= positions, start, 0))

    startr[...] = lax.fori_loop(0, starts.shape[0], latest, jnp.zeros((1, t), jnp.int32))

    def scores(b, own):
        for h in range(heads):
            for c in range(chunks):
                lanes = slice(c * CHUNK, (c + 1) * CHUNK)
                rows = (c + 1) * CHUNK if own else t
                slot = (h * chunks + c) % 2
                s = dot(kb[b, :rows, :], qt[h, :, lanes]) * to_exp2
                j = lax.broadcasted_iota(jnp.int32, (rows, CHUNK), 0)
                visible = j >= startr[:, lanes] - (me - b) * t
                if own:
                    p = lax.broadcasted_iota(jnp.int32, (rows, CHUNK), 1) + c * CHUNK
                    visible = visible & (j <= p)
                s = jnp.where(visible, s, NEG)
                sbuf[slot, :rows, :] = s
                top = jnp.max(s, axis=0, keepdims=True)
                if not own:
                    before = mrun[h:h + 1, lanes]
                    top = jnp.maximum(before, top)
                e = jnp.exp2(sbuf[slot, :rows, :] - top)
                total = jnp.sum(e, axis=0, keepdims=True)
                if not own:
                    total = total + trun[h:h + 1, lanes] * jnp.exp2(before - top)
                eb[b, h, :rows, lanes] = e.astype(BF16)
                if rows < t:
                    eb[b, h, rows:, lanes] = jnp.zeros((t - rows, CHUNK), BF16)
                mrun[h:h + 1, lanes] = top
                mblk[b, h:h + 1, lanes] = top
                trun[h:h + 1, lanes] = total

    def grad_probs(b, own):
        for h in range(heads):
            for c in range(chunks):
                lanes = slice(c * CHUNK, (c + 1) * CHUNK)
                rows = (c + 1) * CHUNK if own else t
                x = dot(vb[b, :rows, :], gt[h, :, lanes])
                gp[b, h, :rows, lanes] = x
                dblk[b, h:h + 1, lanes] = jnp.sum(
                    eb[b, h, :rows, lanes].astype(F32) * x, axis=0, keepdims=True
                )

    def grad_scores(b, own):
        for h in range(heads):
            for c in range(chunks):
                lanes = slice(c * CHUNK, (c + 1) * CHUNK)
                rows = (c + 1) * CHUNK if own else t
                eb[b, h, :rows, lanes] = (
                    eb[b, h, :rows, lanes].astype(F32) * (gp[b, h, :rows, lanes] - dlt[h:h + 1, lanes])
                ).astype(BF16)

    def contract(b, rights, factor):
        total = None
        for h in range(heads):
            right = (rights[h].astype(F32) * (scl[b, h:h + 1, :] * factor)).astype(BF16)
            term = dot_t(eb[b, h], right)
            total = term if total is None else total + term
        return total

    def grad_query(b, first):
        for h in range(heads):
            for c in range(chunks):
                lanes = slice(c * CHUNK, (c + 1) * CHUNK)
                x = dot(kt[b], eb[b, h, :, lanes]) * (scl[b, h:h + 1, lanes] * unit)
                dqt[h, :, lanes] = x if first else dqt[h, :, lanes] + x

    scores(0, True)
    loads[2].wait()
    loads[3].wait()
    for h in range(heads):
        gt[h] = gv[:, h * d:(h + 1) * d].T
    grad_probs(0, True)

    def arrive(step):
        return jnp.where(jnp.logical_and(odd == 1, step > 1), 5 - step, step)

    def k_step(step, carry):
        b = arrive(step)

        @pl.when(jnp.logical_and(even, step == 1))
        def _():
            for r in range(PIECES):
                pass_on_even(keys, r)
            send_own_link(values)
            send_own_partner(values)

        @pl.when(jnp.logical_and(odd == 1, step == 2))
        def _():
            for r in range(PIECES):
                pass_on_odd(keys, r)
            send_own_link(values)

        @pl.when(step != 1 + odd)
        def _():
            await_block(keys, b)

        scores(b, False)
        kt[b] = kb[b].T
        return carry

    lax.fori_loop(1, HOPS + 1, k_step, 0)

    @pl.when(even)
    def _():
        pass_on_even(values, 0)

    for h in range(heads):
        inverse = 1.0 / trun[h:h + 1, :]
        for b in range(HOPS + 1):
            scl[b, h:h + 1, :] = jnp.exp2(mblk[b, h:h + 1, :] - mrun[h:h + 1, :]) * inverse

    def off_of(step):
        on_odd = jnp.where(step == 2, 3, 2 - step)
        return jnp.where(even, 3 - step, on_odd)

    sides = {"v": (shv, rbv, sent_v, got_v), "k": (shk, rbk, sent_k, got_k)}

    def back(side, off, r):
        send_buf, land, send, recv = sides[side]
        step = jnp.where(even, jnp.where(off == 1, -1, jnp.where(off == 2, 1, -2)), jnp.where(off == 3, -3, -1))
        slot = jnp.where(off == 1, 2, jnp.where(off == 2, 0, jnp.where(even, 1, 3)))
        rows = pl.ds(r * piece, piece)
        return pltpu.make_async_remote_copy(
            src_ref=send_buf.at[off, rows], dst_ref=land.at[slot, rows],
            send_sem=send.at[off, r], recv_sem=recv.at[slot, r],
            device_id=dev(step), device_id_type=MESH,
        )

    def send_back(side, off):
        for r in range(PIECES):
            back(side, off, r).start()

    def landed(side, slot, r):
        send_buf, land, send, recv = sides[side]
        rows = pl.ds(r * piece, piece)
        pltpu.make_async_remote_copy(
            src_ref=land.at[slot, rows], dst_ref=land.at[slot, rows],
            send_sem=send.at[0, r], recv_sem=recv.at[slot, r],
            device_id=dev(1), device_id_type=MESH,
        ).wait_recv()

    def share_step(side, rights, factor, extra):
        def run(step, carry):
            off = off_of(step)
            if side == "k":
                grad_scores(off, False)
            sides[side][0][off] = contract(off, rights, factor).astype(BF16)

            @pl.when(step < 2)
            def _():
                send_back(side, off)

            if extra is not None:
                extra(step)

            return carry

        lax.fori_loop(0, HOPS, run, 0)

    def combine(side, off, slots, r):
        send_buf, land, send, recv = sides[side]
        rows = slice(r * piece, (r + 1) * piece)
        total = send_buf[off, rows].astype(F32)
        for slot in slots:
            landed(side, slot, r)
            total = total + land[slot, rows].astype(F32)
        send_buf[off, rows] = total.astype(BF16)
        back(side, off, r).start()

    def combine_odd(side, r):
        combine(side, 3, (0,), r)

    def combine_even(side, r):
        combine(side, 1, (0, 1), r)

    def relay_second(step):
        @pl.when(jnp.logical_and(even, step == 1))
        def _():
            pass_on_even(values, 1)

    share_step("v", gt, 1.0, relay_second)
    own_v[...] = contract(0, gt, 1.0)

    def v_step(step, carry):
        b = arrive(step)

        @pl.when(jnp.logical_and(even, step == 1))
        def _():
            pass_on_even(values, 2)

        @pl.when(jnp.logical_and(odd == 1, step == 2))
        def _():
            pass_on_odd(values, 0)
            pass_on_odd(values, 1)
            for r in range(PIECES):
                combine_odd("v", r)
            pass_on_odd(values, 2)

        @pl.when(jnp.logical_and(even, step == 3))
        def _():
            for r in range(PIECES):
                combine_even("v", r)

        @pl.when(step != 1 + odd)
        def _():
            await_block(values, b)

        grad_probs(b, False)
        return carry

    lax.fori_loop(1, HOPS + 1, v_step, 0)

    for h in range(heads):
        delta = None
        for b in range(HOPS + 1):
            term = dblk[b, h:h + 1, :] * scl[b, h:h + 1, :]
            delta = term if delta is None else delta + term
        dlt[h:h + 1, :] = delta

    share_step("k", qt, unit, None)

    @pl.when(odd == 1)
    def _():
        for r in range(PIECES):
            combine_odd("k", r)

    grad_scores(0, True)
    own_k[...] = contract(0, qt, unit)

    for b in range(HOPS + 1):
        @pl.when(jnp.logical_and(even, b < PIECES))
        def _():
            combine_even("k", min(b, PIECES - 1))

        grad_query(b, b == 0)

    for h in range(heads):
        dq_out[:, h * d:(h + 1) * d] = dqt[h].T.astype(BF16)

    for side, own, column in (("v", own_v, d), ("k", own_k, 0)):
        land = sides[side][1]
        for r in range(PIECES):
            landed(side, 2, r)
        own[...] = own[...] + land[2].astype(F32)

        @pl.when(even)
        def _():
            for r in range(PIECES):
                landed(side, 3, r)
            own[...] = own[...] + land[3].astype(F32)

        dkv_out[:, column:column + d] = own[...].astype(BF16)

    for r in range(PIECES):
        for group in (keys, values):
            to_link(group, r).wait_send()
            relay_partner(group, r).wait_send()

            @pl.when(even)
            def _():
                to_partner(group, r).wait_send()
                relay_link(group, r).wait_send()

        for side in ("v", "k"):
            for off in range(1, HOPS + 1):
                back(side, off, r).wait_send()


def shards(n, query, key_value, d_out, doc_starts):
    t, width = key_value.shape
    d = width // 2
    heads = query.shape[1] // d
    blocks = HOPS + 1
    hbm = pl.BlockSpec(memory_space=pltpu.HBM)
    vmem = pltpu.VMEM
    dma = pltpu.SemaphoreType.DMA
    return pl.pallas_call(
        functools.partial(kernel, n),
        out_shape=(
            jax.ShapeDtypeStruct(query.shape, BF16),
            jax.ShapeDtypeStruct(key_value.shape, BF16),
        ),
        in_specs=[hbm, hbm, hbm, hbm],
        out_specs=(pl.BlockSpec(memory_space=vmem), pl.BlockSpec(memory_space=vmem)),
        scratch_shapes=[
            pltpu.SMEM(doc_starts.shape, jnp.int32),
            vmem((t, heads * d), BF16), vmem((t, heads * d), BF16),
            vmem((blocks, t, d), BF16), vmem((blocks, t, d), BF16),
            vmem((heads, d, t), BF16), vmem((heads, d, t), BF16), vmem((blocks, d, t), BF16),
            vmem((1, t), jnp.int32),
            vmem((blocks, heads, t, t), BF16), vmem((blocks, heads, t, t), F32),
            vmem((2, t, CHUNK), F32),
            vmem((heads, t), F32), vmem((heads, t), F32),
            vmem((blocks, heads, t), F32), vmem((blocks, heads, t), F32), vmem((blocks, heads, t), F32),
            vmem((heads, t), F32), vmem((heads, d, t), F32),
            vmem((t, d), F32), vmem((t, d), F32),
            vmem((blocks, t, d), BF16), vmem((blocks, t, d), BF16),
            vmem((blocks, t, d), BF16), vmem((blocks, t, d), BF16),
            dma((5,)), *[dma((4, PIECES)) for _ in range(8)],
        ],
        compiler_params=pltpu.CompilerParams(
            collective_id=0, has_side_effects=True, vmem_limit_bytes=60 * 1024 * 1024
        ),
    )(query, key_value, d_out, doc_starts)


def solution(mesh):
    placed = (P("ctx", "head"), P("ctx", "head"), P("ctx", "head"), P("head"))
    return jax.shard_map(
        functools.partial(shards, mesh.shape["ctx"]),
        mesh=mesh,
        in_specs=placed,
        out_specs=(P("ctx", "head"), P("ctx", "head")),
        check_vma=False,
    )
```

```python
import functools

import jax
import jax.numpy as jnp
from jax import lax
from jax.experimental import pallas as pl
from jax.experimental.pallas import tpu as pltpu
from jax.sharding import PartitionSpec as P

MESH = pl.DeviceIdType.MESH
HOPS = 3
CHUNK = 256
PIECES = 3
NEG = -1e30
F32 = jnp.float32
BF16 = jnp.bfloat16


def dot(a, b):
    return lax.dot_general(a, b, (((1,), (0,)), ((), ())), preferred_element_type=F32)


def dot_t(a, b):
    return lax.dot_general(a, b, (((1,), (1,)), ((), ())), preferred_element_type=F32)


def kernel(
    n, q_hbm, kv_hbm, g_hbm, starts_hbm, dq_out, dkv_out,
    starts, qv, gv, kb, vb, qt, gt, kt, bias, docs, eb, gp, sbuf, mrun, trun, mblk, dblk, scl, dlt, dqt,
    own_v, own_k, shv, shk, rbv, rbk,
    load_sem, sk, sv, rk, rv, sent_v, sent_k, got_v, got_k,
):
    me = lax.axis_index("ctx")
    row = lax.axis_index("head")
    odd = lax.rem(me, 2)
    even = odd == 0
    t, d = kb.shape[1], kb.shape[2]
    heads = qt.shape[0]
    chunks = t // CHUNK
    unit = d ** (-0.5)
    to_exp2 = unit * 1.4426950408889634

    def dev(step):
        return (lax.rem(me + step + n, n), row)

    loads = [
        pltpu.make_async_copy(kv_hbm.at[:, pl.ds(0, d)], kb.at[0], load_sem.at[0]),
        pltpu.make_async_copy(q_hbm, qv, load_sem.at[1]),
        pltpu.make_async_copy(kv_hbm.at[:, pl.ds(d, d)], vb.at[0], load_sem.at[2]),
        pltpu.make_async_copy(g_hbm, gv, load_sem.at[3]),
        pltpu.make_async_copy(starts_hbm, starts, load_sem.at[4]),
    ]
    for load in loads:
        load.start()

    barrier = pltpu.get_barrier_semaphore()

    has_prev = me >= 2
    has_next = me < n - 2

    def greet(partner, senders, receivers):
        def hail(step):
            pl.semaphore_signal(barrier, inc=1, device_id=dev(step), device_id_type=MESH)

        hail(partner[0])

        @pl.when(has_prev)
        def _():
            for step in senders:
                hail(step)

        pl.semaphore_wait(barrier, jnp.where(has_next, 1 + len(receivers), 1))

    @pl.when(even)
    def _():
        greet((1,), (-1, -2), (3, 2))

    @pl.when(odd == 1)
    def _():
        greet((-1,), (-3,), (1,))

    piece = t // PIECES
    keys = (kb, sk, rk)
    values = (vb, sv, rv)

    def forward(group, which, source, slot, step, r):
        buf, send, recv = group
        rows = pl.ds(r * piece, piece)
        return pltpu.make_async_remote_copy(
            src_ref=buf.at[source, rows], dst_ref=buf.at[slot, rows],
            send_sem=send.at[which, r], recv_sem=recv.at[slot, r],
            device_id=dev(step), device_id_type=MESH,
        )

    def to_link(group, r):
        return forward(group, 0, 0, 3 - 2 * odd, 3 - 2 * odd, r)

    def to_partner(group, r):
        return forward(group, 1, 0, 1, 1, r)

    def relay_partner(group, r):
        return forward(group, 2, 1 + 2 * odd, 2, 1 - 2 * odd, r)

    def relay_link(group, r):
        return forward(group, 3, 1, 3, 2, r)

    def await_piece(group, slot, r):
        forward(group, 0, 0, slot, 1, r).wait_recv()

    def await_block(group, slot):
        for r in range(PIECES):
            await_piece(group, slot, r)

    def send_own_link(group):
        @pl.when(has_next)
        def _():
            for r in range(PIECES):
                to_link(group, r).start()

    def send_own_partner(group):
        for r in range(PIECES):
            to_partner(group, r).start()

    def pass_on_even(group, r):
        @pl.when(has_prev)
        def _():
            await_piece(group, 1, r)

            @pl.when(has_next)
            def _():
                relay_link(group, r).start()

            relay_partner(group, r).start()

    def pass_on_odd(group, r):
        @pl.when(has_prev)
        def _():
            await_piece(group, 3, r)
            relay_partner(group, r).start()

    loads[0].wait()
    send_own_link(keys)

    @pl.when(even)
    def _():
        send_own_partner(keys)

    loads[1].wait()
    loads[4].wait()
    for h in range(heads):
        qt[h] = qv[:, h * d:(h + 1) * d].T
    kt[0] = kb[0].T

    for b in range(1, HOPS + 1):
        @pl.when(me < b)
        def _():
            kb[b] = jnp.zeros((t, d), BF16)
            vb[b] = jnp.zeros((t, d), BF16)

    count = starts.shape[1]
    first = jnp.broadcast_to(starts[...].astype(F32), (count, count))
    lane = lax.broadcasted_iota(jnp.int32, (count, count), 1)
    after = jnp.where(lane == count - 1, float(n * t), pltpu.roll(first, count - 1, 1))
    first_q, after_q = first.T[:, :1], after.T[:, :1]
    at = (me * t + lax.broadcasted_iota(jnp.int32, (count, t), 1)).astype(F32)
    bias[...] = jnp.where((at >= first_q) & (at < after_q), 0.0, NEG).astype(BF16)

    def mark_docs(b):
        j = ((me - b) * t + lax.broadcasted_iota(jnp.int32, (t, count), 0)).astype(F32)
        inside = (j >= first[:1]) & (j < after[:1])
        docs[b] = jnp.where(inside | (j < 0.0), 1.0, 0.0).astype(BF16)

    for b in range(HOPS + 1):
        mark_docs(b)

    def scores(b, own):
        for h in range(heads):
            for c in range(chunks):
                lanes = slice(c * CHUNK, (c + 1) * CHUNK)
                rows = (c + 1) * CHUNK if own else t
                slot = (h * chunks + c) % 2
                left = jnp.concatenate([kb[b, :rows, :], docs[b, :rows, :]], axis=1)
                right = jnp.concatenate([qt[h, :, lanes], bias[:, lanes]], axis=0)
                s = dot(left, right) * to_exp2
                if own:
                    j = lax.broadcasted_iota(jnp.int32, (rows, CHUNK), 0)
                    p = lax.broadcasted_iota(jnp.int32, (rows, CHUNK), 1) + c * CHUNK
                    s = jnp.where(j <= p, s, NEG)
                sbuf[slot, :rows, :] = s
                top = jnp.max(s, axis=0, keepdims=True)
                if not own:
                    before = mrun[h:h + 1, lanes]
                    top = jnp.maximum(before, top)
                e = jnp.exp2(sbuf[slot, :rows, :] - top)
                total = jnp.sum(e, axis=0, keepdims=True)
                if not own:
                    total = total + trun[h:h + 1, lanes] * jnp.exp2(before - top)
                eb[b, h, :rows, lanes] = e.astype(BF16)
                if rows < t:
                    eb[b, h, rows:, lanes] = jnp.zeros((t - rows, CHUNK), BF16)
                mrun[h:h + 1, lanes] = top
                mblk[b, h:h + 1, lanes] = top
                trun[h:h + 1, lanes] = total

    def grad_probs(b, own):
        for h in range(heads):
            for c in range(chunks):
                lanes = slice(c * CHUNK, (c + 1) * CHUNK)
                rows = (c + 1) * CHUNK if own else t
                x = dot(vb[b, :rows, :], gt[h, :, lanes])
                gp[b, h, :rows, lanes] = x
                dblk[b, h:h + 1, lanes] = jnp.sum(
                    eb[b, h, :rows, lanes].astype(F32) * x, axis=0, keepdims=True
                )

    def grad_scores(b, own):
        for h in range(heads):
            for c in range(chunks):
                lanes = slice(c * CHUNK, (c + 1) * CHUNK)
                rows = (c + 1) * CHUNK if own else t
                eb[b, h, :rows, lanes] = (
                    eb[b, h, :rows, lanes].astype(F32) * (gp[b, h, :rows, lanes] - dlt[h:h + 1, lanes])
                ).astype(BF16)

    def contract(b, rights, factor):
        total = None
        for h in range(heads):
            right = (rights[h].astype(F32) * (scl[b, h:h + 1, :] * factor)).astype(BF16)
            term = dot_t(eb[b, h], right)
            total = term if total is None else total + term
        return total

    def grad_query(b, first):
        for h in range(heads):
            for c in range(chunks):
                lanes = slice(c * CHUNK, (c + 1) * CHUNK)
                x = dot(kt[b], eb[b, h, :, lanes]) * (scl[b, h:h + 1, lanes] * unit)
                dqt[h, :, lanes] = x if first else dqt[h, :, lanes] + x

    scores(0, True)
    loads[2].wait()
    loads[3].wait()
    for h in range(heads):
        gt[h] = gv[:, h * d:(h + 1) * d].T
    grad_probs(0, True)

    def arrive(step):
        return jnp.where(jnp.logical_and(odd == 1, step > 1), 5 - step, step)

    def k_step(step, carry):
        b = arrive(step)

        @pl.when(jnp.logical_and(even, step == 1))
        def _():
            for r in range(PIECES):
                pass_on_even(keys, r)
            send_own_link(values)
            send_own_partner(values)

        @pl.when(jnp.logical_and(odd == 1, step == 2))
        def _():
            for r in range(PIECES):
                pass_on_odd(keys, r)
            send_own_link(values)

        @pl.when(jnp.logical_and(step != 1 + odd, me >= b))
        def _():
            await_block(keys, b)

        scores(b, False)
        kt[b] = kb[b].T
        return carry

    lax.fori_loop(1, HOPS + 1, k_step, 0)

    @pl.when(even)
    def _():
        pass_on_even(values, 0)

    for h in range(heads):
        inverse = 1.0 / trun[h:h + 1, :]
        for b in range(HOPS + 1):
            scl[b, h:h + 1, :] = jnp.exp2(mblk[b, h:h + 1, :] - mrun[h:h + 1, :]) * inverse

    def off_of(step):
        on_odd = jnp.where(step == 2, 3, 2 - step)
        return jnp.where(even, 3 - step, on_odd)

    sides = {"v": (shv, rbv, sent_v, got_v), "k": (shk, rbk, sent_k, got_k)}

    def back(side, off, r):
        send_buf, land, send, recv = sides[side]
        step = jnp.where(even, jnp.where(off == 1, -1, jnp.where(off == 2, 1, -2)), jnp.where(off == 3, -3, -1))
        slot = jnp.where(off == 1, 2, jnp.where(off == 2, 0, jnp.where(even, 1, 3)))
        rows = pl.ds(r * piece, piece)
        return pltpu.make_async_remote_copy(
            src_ref=send_buf.at[off, rows], dst_ref=land.at[slot, rows],
            send_sem=send.at[off, r], recv_sem=recv.at[slot, r],
            device_id=dev(step), device_id_type=MESH,
        )

    def send_back(side, off):
        for r in range(PIECES):
            back(side, off, r).start()

    def landed(side, slot, r):
        send_buf, land, send, recv = sides[side]
        rows = pl.ds(r * piece, piece)
        pltpu.make_async_remote_copy(
            src_ref=land.at[slot, rows], dst_ref=land.at[slot, rows],
            send_sem=send.at[0, r], recv_sem=recv.at[slot, r],
            device_id=dev(1), device_id_type=MESH,
        ).wait_recv()

    def share_step(side, rights, factor, extra):
        def run(step, carry):
            off = off_of(step)
            if side == "k":
                grad_scores(off, False)
            sides[side][0][off] = contract(off, rights, factor).astype(BF16)

            @pl.when(jnp.logical_and(step < 2, me >= off))
            def _():
                send_back(side, off)

            if extra is not None:
                extra(step)

            return carry

        lax.fori_loop(0, HOPS, run, 0)

    def add_landed(side, off, slot, r):
        send_buf, land, send, recv = sides[side]
        rows = slice(r * piece, (r + 1) * piece)
        landed(side, slot, r)
        total = send_buf[off, rows].astype(F32) + land[slot, rows].astype(F32)
        send_buf[off, rows] = total.astype(BF16)

    def combine_odd(side, r):
        @pl.when(has_prev)
        def _():
            add_landed(side, 3, 0, r)
            back(side, 3, r).start()

    def combine_even(side, r):
        send_buf, land, send, recv = sides[side]
        rows = slice(r * piece, (r + 1) * piece)

        @pl.when(jnp.logical_and(has_prev, has_next))
        def _():
            landed(side, 0, r)
            landed(side, 1, r)
            total = send_buf[1, rows].astype(F32) + land[0, rows].astype(F32)
            send_buf[1, rows] = (total + land[1, rows].astype(F32)).astype(BF16)

        @pl.when(jnp.logical_and(has_prev, jnp.logical_not(has_next)))
        def _():
            add_landed(side, 1, 0, r)

        @pl.when(has_prev)
        def _():
            back(side, 1, r).start()

    def relay_second(step):
        @pl.when(jnp.logical_and(even, step == 1))
        def _():
            pass_on_even(values, 1)

    share_step("v", gt, 1.0, relay_second)
    own_v[...] = contract(0, gt, 1.0)

    def v_step(step, carry):
        b = arrive(step)

        @pl.when(jnp.logical_and(even, step == 1))
        def _():
            pass_on_even(values, 2)

        @pl.when(jnp.logical_and(odd == 1, step == 2))
        def _():
            pass_on_odd(values, 0)
            pass_on_odd(values, 1)
            for r in range(PIECES):
                combine_odd("v", r)
            pass_on_odd(values, 2)

        @pl.when(jnp.logical_and(even, step == 3))
        def _():
            for r in range(PIECES):
                combine_even("v", r)

        @pl.when(jnp.logical_and(step != 1 + odd, me >= b))
        def _():
            await_block(values, b)

        grad_probs(b, False)
        return carry

    lax.fori_loop(1, HOPS + 1, v_step, 0)

    for h in range(heads):
        delta = None
        for b in range(HOPS + 1):
            term = dblk[b, h:h + 1, :] * scl[b, h:h + 1, :]
            delta = term if delta is None else delta + term
        dlt[h:h + 1, :] = delta

    share_step("k", qt, unit, None)

    @pl.when(odd == 1)
    def _():
        for r in range(PIECES):
            combine_odd("k", r)

    grad_scores(0, True)
    own_k[...] = contract(0, qt, unit)

    for b in range(HOPS + 1):
        @pl.when(jnp.logical_and(even, b < PIECES))
        def _():
            combine_even("k", min(b, PIECES - 1))

        grad_query(b, b == 0)

    for h in range(heads):
        dq_out[:, h * d:(h + 1) * d] = dqt[h].T.astype(BF16)

    for side, own, column in (("v", own_v, d), ("k", own_k, 0)):
        land = sides[side][1]

        @pl.when(jnp.logical_or(even, has_next))
        def _():
            for r in range(PIECES):
                landed(side, 2, r)
            own[...] = own[...] + land[2].astype(F32)

        @pl.when(jnp.logical_and(even, has_next))
        def _():
            for r in range(PIECES):
                landed(side, 3, r)
            own[...] = own[...] + land[3].astype(F32)

        dkv_out[:, column:column + d] = own[...].astype(BF16)

    for r in range(PIECES):
        for group in (keys, values):
            @pl.when(has_next)
            def _():
                to_link(group, r).wait_send()

            @pl.when(has_prev)
            def _():
                relay_partner(group, r).wait_send()

            @pl.when(even)
            def _():
                to_partner(group, r).wait_send()

            @pl.when(jnp.logical_and(even, jnp.logical_and(has_prev, has_next)))
            def _():
                relay_link(group, r).wait_send()

        for side in ("v", "k"):
            for off in range(1, HOPS + 1):
                @pl.when(me >= off)
                def _():
                    back(side, off, r).wait_send()


def shards(n, query, key_value, d_out, doc_starts):
    t, width = key_value.shape
    d = width // 2
    heads = query.shape[1] // d
    blocks = HOPS + 1
    hbm = pl.BlockSpec(memory_space=pltpu.HBM)
    vmem = pltpu.VMEM
    dma = pltpu.SemaphoreType.DMA
    return pl.pallas_call(
        functools.partial(kernel, n),
        out_shape=(
            jax.ShapeDtypeStruct(query.shape, BF16),
            jax.ShapeDtypeStruct(key_value.shape, BF16),
        ),
        in_specs=[hbm, hbm, hbm, hbm],
        out_specs=(pl.BlockSpec(memory_space=vmem), pl.BlockSpec(memory_space=vmem)),
        scratch_shapes=[
            vmem((1, doc_starts.shape[0]), jnp.int32),
            vmem((t, heads * d), BF16), vmem((t, heads * d), BF16),
            vmem((blocks, t, d), BF16), vmem((blocks, t, d), BF16),
            vmem((heads, d, t), BF16), vmem((heads, d, t), BF16), vmem((blocks, d, t), BF16),
            vmem((doc_starts.shape[0], t), BF16), vmem((blocks, t, doc_starts.shape[0]), BF16),
            vmem((blocks, heads, t, t), BF16), vmem((blocks, heads, t, t), F32),
            vmem((2, t, CHUNK), F32),
            vmem((heads, t), F32), vmem((heads, t), F32),
            vmem((blocks, heads, t), F32), vmem((blocks, heads, t), F32), vmem((blocks, heads, t), F32),
            vmem((heads, t), F32), vmem((heads, d, t), F32),
            vmem((t, d), F32), vmem((t, d), F32),
            vmem((blocks, t, d), BF16), vmem((blocks, t, d), BF16),
            vmem((blocks, t, d), BF16), vmem((blocks, t, d), BF16),
            dma((5,)), *[dma((4, PIECES)) for _ in range(8)],
        ],
        compiler_params=pltpu.CompilerParams(
            collective_id=0, has_side_effects=True, vmem_limit_bytes=50 * 1024 * 1024
        ),
    )(*[pltpu.with_memory_space_constraint(x, pltpu.HBM) for x in (query, key_value, d_out, doc_starts.reshape(1, -1))])


def solution(mesh):
    placed = (P("ctx", "head"), P("ctx", "head"), P("ctx", "head"), P("head"))
    return jax.shard_map(
        functools.partial(shards, mesh.shape["ctx"]),
        mesh=mesh,
        in_specs=placed,
        out_specs=(P("ctx", "head"), P("ctx", "head")),
        check_vma=False,
    )
```

```python
import functools

import jax
import jax.numpy as jnp
from jax import lax
from jax.experimental import pallas as pl
from jax.experimental.pallas import tpu as pltpu
from jax.sharding import PartitionSpec as P

MESH = pl.DeviceIdType.MESH
HOPS = 3
CHUNK = 256
PIECES = 3
COLUMN = 16
NEG = -1e30
F32 = jnp.float32
BF16 = jnp.bfloat16


def dot(a, b):
    return lax.dot_general(a, b, (((1,), (0,)), ((), ())), preferred_element_type=F32)


def dot_t(a, b):
    return lax.dot_general(a, b, (((1,), (1,)), ((), ())), preferred_element_type=F32)


def kernel(
    n, q_hbm, kv_hbm, g_hbm, starts_hbm, dq_out, dkv_out,
    starts, qv, gv, kb, vb, qt, gt, kt, bias, docs, eb, gp, sbuf, mrun, trun, mblk, dblk, scl, dlt, dqt,
    own_v, own_k, shv, shk, rbv, rbk,
    load_sem, sk, sv, rk, rv, sent_v, sent_k, got_v, got_k,
):
    me = lax.axis_index("ctx")
    row = lax.axis_index("head")
    odd = lax.rem(me, 2)
    even = odd == 0
    t, d = kb.shape[1], kb.shape[2]
    heads = qt.shape[0]
    chunks = t // CHUNK
    unit = d ** (-0.5)
    to_exp2 = unit * 1.4426950408889634

    def dev(step):
        return (lax.rem(me + step + n, n), row)

    loads = [
        pltpu.make_async_copy(kv_hbm.at[:, pl.ds(0, d)], kb.at[0], load_sem.at[0]),
        pltpu.make_async_copy(q_hbm, qv, load_sem.at[1]),
        pltpu.make_async_copy(kv_hbm.at[:, pl.ds(d, d)], vb.at[0], load_sem.at[2]),
        pltpu.make_async_copy(g_hbm, gv, load_sem.at[3]),
        pltpu.make_async_copy(starts_hbm, starts, load_sem.at[4]),
    ]
    for load in loads:
        load.start()

    barrier = pltpu.get_barrier_semaphore()

    first_chip = lax.rem(me, COLUMN) < 2
    second_even = lax.rem(me, COLUMN) == 2
    late = lax.rem(me, COLUMN) == 6
    has_prev = me >= 2
    has_next = me < n - 2

    def greet(partner, senders, receivers):
        def hail(step):
            pl.semaphore_signal(barrier, inc=1, device_id=dev(step), device_id_type=MESH)

        hail(partner[0])

        @pl.when(has_prev)
        def _():
            for step in senders:
                hail(step)

        pl.semaphore_wait(barrier, jnp.where(has_next, 1 + len(receivers), 1))

    @pl.when(even)
    def _():
        greet((1,), (-1, -2), (3, 2))

    @pl.when(odd == 1)
    def _():
        greet((-1,), (-3,), (1,))

    piece = t // PIECES
    keys = (kb, sk, rk)
    values = (vb, sv, rv)

    def forward(group, which, source, slot, step, r):
        buf, send, recv = group
        rows = pl.ds(r * piece, piece)
        return pltpu.make_async_remote_copy(
            src_ref=buf.at[source, rows], dst_ref=buf.at[slot, rows],
            send_sem=send.at[which, r], recv_sem=recv.at[slot, r],
            device_id=dev(step), device_id_type=MESH,
        )

    def to_link(group, r):
        return forward(group, 0, 0, 3 - 2 * odd, 3 - 2 * odd, r)

    def to_partner(group, r):
        return forward(group, 1, 0, 1, 1, r)

    def relay_partner(group, r):
        return forward(group, 2, 1 + 2 * odd, 2, 1 - 2 * odd, r)

    def relay_link(group, r):
        return forward(group, 3, 1, 3, 2, r)

    def await_piece(group, slot, r):
        forward(group, 0, 0, slot, 1, r).wait_recv()

    def await_block(group, slot):
        for r in range(PIECES):
            await_piece(group, slot, r)

    def send_own_link(group):
        @pl.when(has_next)
        def _():
            for r in range(PIECES):
                to_link(group, r).start()

    def send_own_partner(group):
        for r in range(PIECES):
            to_partner(group, r).start()

    def pass_on_even(group, r):
        @pl.when(has_prev)
        def _():
            await_piece(group, 1, r)

            @pl.when(has_next)
            def _():
                relay_link(group, r).start()

            relay_partner(group, r).start()

    def pass_on_odd(group, r):
        @pl.when(has_prev)
        def _():
            await_piece(group, 3, r)
            relay_partner(group, r).start()

    loads[0].wait()
    send_own_link(keys)

    @pl.when(even)
    def _():
        send_own_partner(keys)

    loads[2].wait()

    @pl.when(first_chip)
    def _():
        send_own_link(values)

        @pl.when(even)
        def _():
            send_own_partner(values)

    loads[1].wait()
    loads[4].wait()
    for h in range(heads):
        qt[h] = qv[:, h * d:(h + 1) * d].T
    kt[0] = kb[0].T

    for b in range(1, HOPS + 1):
        @pl.when(me < b)
        def _():
            kb[b] = jnp.zeros((t, d), BF16)
            vb[b] = jnp.zeros((t, d), BF16)

    count = starts.shape[1]
    first = jnp.broadcast_to(starts[...].astype(F32), (count, count))
    lane = lax.broadcasted_iota(jnp.int32, (count, count), 1)
    after = jnp.where(lane == count - 1, float(n * t), pltpu.roll(first, count - 1, 1))
    first_q, after_q = first.T[:, :1], after.T[:, :1]
    at = (me * t + lax.broadcasted_iota(jnp.int32, (count, t), 1)).astype(F32)
    bias[...] = jnp.where((at >= first_q) & (at < after_q), 0.0, NEG).astype(BF16)

    def mark_docs(b):
        j = ((me - b) * t + lax.broadcasted_iota(jnp.int32, (t, count), 0)).astype(F32)
        inside = (j >= first[:1]) & (j < after[:1])
        docs[b] = jnp.where(inside | (j < 0.0), 1.0, 0.0).astype(BF16)

    for b in range(HOPS + 1):
        mark_docs(b)

    def scores(b, own):
        for h in range(heads):
            for c in range(chunks):
                lanes = slice(c * CHUNK, (c + 1) * CHUNK)
                rows = (c + 1) * CHUNK if own else t
                slot = (h * chunks + c) % 2
                left = jnp.concatenate([kb[b, :rows, :], docs[b, :rows, :]], axis=1)
                right = jnp.concatenate([qt[h, :, lanes], bias[:, lanes]], axis=0)
                s = dot(left, right) * to_exp2
                if own:
                    j = lax.broadcasted_iota(jnp.int32, (rows, CHUNK), 0)
                    p = lax.broadcasted_iota(jnp.int32, (rows, CHUNK), 1) + c * CHUNK
                    s = jnp.where(j <= p, s, NEG)
                sbuf[slot, :rows, :] = s
                top = jnp.max(s, axis=0, keepdims=True)
                if not own:
                    before = mrun[h:h + 1, lanes]
                    top = jnp.maximum(before, top)
                e = jnp.exp2(sbuf[slot, :rows, :] - top)
                total = jnp.sum(e, axis=0, keepdims=True)
                if not own:
                    total = total + trun[h:h + 1, lanes] * jnp.exp2(before - top)
                eb[b, h, :rows, lanes] = e.astype(BF16)
                if rows < t:
                    eb[b, h, rows:, lanes] = jnp.zeros((t - rows, CHUNK), BF16)
                mrun[h:h + 1, lanes] = top
                mblk[b, h:h + 1, lanes] = top
                trun[h:h + 1, lanes] = total

    def grad_probs(b, own):
        for h in range(heads):
            for c in range(chunks):
                lanes = slice(c * CHUNK, (c + 1) * CHUNK)
                rows = (c + 1) * CHUNK if own else t
                x = dot(vb[b, :rows, :], gt[h, :, lanes])
                gp[b, h, :rows, lanes] = x
                dblk[b, h:h + 1, lanes] = jnp.sum(
                    eb[b, h, :rows, lanes].astype(F32) * x, axis=0, keepdims=True
                )

    def grad_scores(b, own):
        for h in range(heads):
            for c in range(chunks):
                lanes = slice(c * CHUNK, (c + 1) * CHUNK)
                rows = (c + 1) * CHUNK if own else t
                eb[b, h, :rows, lanes] = (
                    eb[b, h, :rows, lanes].astype(F32) * (gp[b, h, :rows, lanes] - dlt[h:h + 1, lanes])
                ).astype(BF16)

    def contract(b, rights, factor):
        total = None
        for h in range(heads):
            right = (rights[h].astype(F32) * (scl[b, h:h + 1, :] * factor)).astype(BF16)
            term = dot_t(eb[b, h], right)
            total = term if total is None else total + term
        return total

    def grad_query(b, first):
        for h in range(heads):
            for c in range(chunks):
                lanes = slice(c * CHUNK, (c + 1) * CHUNK)
                x = dot(kt[b], eb[b, h, :, lanes]) * (scl[b, h:h + 1, lanes] * unit)
                dqt[h, :, lanes] = x if first else dqt[h, :, lanes] + x

    scores(0, True)
    loads[3].wait()
    for h in range(heads):
        gt[h] = gv[:, h * d:(h + 1) * d].T
    grad_probs(0, True)

    def arrive(step):
        return jnp.where(jnp.logical_and(odd == 1, step > 1), 5 - step, step)

    def k_step(step, carry):
        b = arrive(step)

        @pl.when(jnp.logical_and(even, step == 1))
        def _():
            for r in range(PIECES):
                pass_on_even(keys, r)

            @pl.when(jnp.logical_not(first_chip))
            def _():
                send_own_link(values)
                send_own_partner(values)

        @pl.when(jnp.logical_and(odd == 1, step == 2))
        def _():
            for r in range(PIECES):
                pass_on_odd(keys, r)

            @pl.when(jnp.logical_not(first_chip))
            def _():
                send_own_link(values)

        @pl.when(jnp.logical_and(second_even, step == HOPS))
        def _():
            for r in range(PIECES):
                pass_on_even(values, r)

        @pl.when(jnp.logical_and(step != 1 + odd, me >= b))
        def _():
            await_block(keys, b)

        scores(b, False)
        kt[b] = kb[b].T
        return carry

    lax.fori_loop(1, HOPS + 1, k_step, 0)

    usual_even = jnp.logical_and(even, jnp.logical_not(second_even))

    @pl.when(usual_even)
    def _():
        pass_on_even(values, 0)

    for h in range(heads):
        inverse = 1.0 / trun[h:h + 1, :]
        for b in range(HOPS + 1):
            scl[b, h:h + 1, :] = jnp.exp2(mblk[b, h:h + 1, :] - mrun[h:h + 1, :]) * inverse

    def off_of(step):
        on_odd = jnp.where(step == 2, 3, 2 - step)
        return jnp.where(even, 3 - step, on_odd)

    sides = {"v": (shv, rbv, sent_v, got_v), "k": (shk, rbk, sent_k, got_k)}

    def back(side, off, r):
        send_buf, land, send, recv = sides[side]
        step = jnp.where(even, jnp.where(off == 1, -1, jnp.where(off == 2, 1, -2)), jnp.where(off == 3, -3, -1))
        slot = jnp.where(off == 1, 2, jnp.where(off == 2, 0, jnp.where(even, 1, 3)))
        rows = pl.ds(r * piece, piece)
        return pltpu.make_async_remote_copy(
            src_ref=send_buf.at[off, rows], dst_ref=land.at[slot, rows],
            send_sem=send.at[off, r], recv_sem=recv.at[slot, r],
            device_id=dev(step), device_id_type=MESH,
        )

    def send_back(side, off):
        for r in range(PIECES):
            back(side, off, r).start()

    def landed(side, slot, r):
        send_buf, land, send, recv = sides[side]
        rows = pl.ds(r * piece, piece)
        pltpu.make_async_remote_copy(
            src_ref=land.at[slot, rows], dst_ref=land.at[slot, rows],
            send_sem=send.at[0, r], recv_sem=recv.at[slot, r],
            device_id=dev(1), device_id_type=MESH,
        ).wait_recv()

    def share_step(side, rights, factor, extra):
        def run(step, carry):
            off = off_of(step)
            if side == "k":
                grad_scores(off, False)
            sides[side][0][off] = contract(off, rights, factor).astype(BF16)

            @pl.when(jnp.logical_and(step < 2, me >= off))
            def _():
                send_back(side, off)

            if extra is not None:
                extra(step)

            return carry

        lax.fori_loop(0, HOPS, run, 0)

    def add_landed(side, off, slot, r):
        send_buf, land, send, recv = sides[side]
        rows = slice(r * piece, (r + 1) * piece)
        landed(side, slot, r)
        total = send_buf[off, rows].astype(F32) + land[slot, rows].astype(F32)
        send_buf[off, rows] = total.astype(BF16)

    def combine_odd(side, r):
        @pl.when(has_prev)
        def _():
            add_landed(side, 3, 0, r)
            back(side, 3, r).start()

    def combine_even(side, r):
        send_buf, land, send, recv = sides[side]
        rows = slice(r * piece, (r + 1) * piece)

        @pl.when(jnp.logical_and(has_prev, has_next))
        def _():
            landed(side, 0, r)
            landed(side, 1, r)
            total = send_buf[1, rows].astype(F32) + land[0, rows].astype(F32)
            send_buf[1, rows] = (total + land[1, rows].astype(F32)).astype(BF16)

        @pl.when(jnp.logical_and(has_prev, jnp.logical_not(has_next)))
        def _():
            add_landed(side, 1, 0, r)

        @pl.when(has_prev)
        def _():
            back(side, 1, r).start()

    def relay_second(step):
        @pl.when(jnp.logical_and(usual_even, step == 1))
        def _():
            pass_on_even(values, 1)

    share_step("v", gt, 1.0, relay_second)
    own_v[...] = contract(0, gt, 1.0)

    def v_step(step, carry):
        b = arrive(step)

        @pl.when(jnp.logical_and(usual_even, step == 1))
        def _():
            pass_on_even(values, 2)

        @pl.when(jnp.logical_and(odd == 1, step == 2))
        def _():
            pass_on_odd(values, 0)
            pass_on_odd(values, 1)
            for r in range(PIECES):
                combine_odd("v", r)
            pass_on_odd(values, 2)

        @pl.when(jnp.logical_and(jnp.logical_and(even, jnp.logical_not(late)), step == 3))
        def _():
            for r in range(PIECES):
                combine_even("v", r)

        @pl.when(jnp.logical_and(step != 1 + odd, me >= b))
        def _():
            await_block(values, b)

        grad_probs(b, False)
        return carry

    lax.fori_loop(1, HOPS + 1, v_step, 0)

    for h in range(heads):
        delta = None
        for b in range(HOPS + 1):
            term = dblk[b, h:h + 1, :] * scl[b, h:h + 1, :]
            delta = term if delta is None else delta + term
        dlt[h:h + 1, :] = delta

    share_step("k", qt, unit, None)

    @pl.when(jnp.logical_and(even, late))
    def _():
        for r in range(PIECES):
            combine_even("v", r)

    @pl.when(odd == 1)
    def _():
        for r in range(PIECES):
            combine_odd("k", r)


    grad_query(3, True)
    for r in range(PIECES):
        @pl.when(even)
        def _():
            combine_even("k", r)

        if r == 0:
            grad_query(2, False)
        if r == 1:
            grad_query(1, False)
        if r == 2:
            grad_scores(0, True)
            own_k[...] = contract(0, qt, unit)
            grad_query(0, False)

    for h in range(heads):
        dq_out[:, h * d:(h + 1) * d] = dqt[h].T.astype(BF16)

    for side, own, column in (("v", own_v, d), ("k", own_k, 0)):
        land = sides[side][1]

        @pl.when(jnp.logical_or(even, has_next))
        def _():
            for r in range(PIECES):
                landed(side, 2, r)
            own[...] = own[...] + land[2].astype(F32)

        @pl.when(jnp.logical_and(even, has_next))
        def _():
            for r in range(PIECES):
                landed(side, 3, r)
            own[...] = own[...] + land[3].astype(F32)

        dkv_out[:, column:column + d] = own[...].astype(BF16)

    for r in range(PIECES):
        for group in (keys, values):
            @pl.when(has_next)
            def _():
                to_link(group, r).wait_send()

            @pl.when(has_prev)
            def _():
                relay_partner(group, r).wait_send()

            @pl.when(even)
            def _():
                to_partner(group, r).wait_send()

            @pl.when(jnp.logical_and(even, jnp.logical_and(has_prev, has_next)))
            def _():
                relay_link(group, r).wait_send()

        for side in ("v", "k"):
            for off in range(1, HOPS + 1):
                @pl.when(me >= off)
                def _():
                    back(side, off, r).wait_send()


def shards(n, query, key_value, d_out, doc_starts):
    t, width = key_value.shape
    d = width // 2
    heads = query.shape[1] // d
    blocks = HOPS + 1
    hbm = pl.BlockSpec(memory_space=pltpu.HBM)
    vmem = pltpu.VMEM
    dma = pltpu.SemaphoreType.DMA
    made = pl.pallas_call(
        functools.partial(kernel, n),
        out_shape=(
            jax.ShapeDtypeStruct(query.shape, BF16),
            jax.ShapeDtypeStruct(key_value.shape, BF16),
        ),
        in_specs=[hbm, hbm, hbm, hbm],
        out_specs=(pl.BlockSpec(memory_space=vmem), pl.BlockSpec(memory_space=vmem)),
        scratch_shapes=[
            vmem((1, doc_starts.shape[0]), jnp.int32),
            vmem((t, heads * d), BF16), vmem((t, heads * d), BF16),
            vmem((blocks, t, d), BF16), vmem((blocks, t, d), BF16),
            vmem((heads, d, t), BF16), vmem((heads, d, t), BF16), vmem((blocks, d, t), BF16),
            vmem((doc_starts.shape[0], t), BF16), vmem((blocks, t, doc_starts.shape[0]), BF16),
            vmem((blocks, heads, t, t), BF16), vmem((blocks, heads, t, t), F32),
            vmem((2, t, CHUNK), F32),
            vmem((heads, t), F32), vmem((heads, t), F32),
            vmem((blocks, heads, t), F32), vmem((blocks, heads, t), F32), vmem((blocks, heads, t), F32),
            vmem((heads, t), F32), vmem((heads, d, t), F32),
            vmem((t, d), F32), vmem((t, d), F32),
            vmem((blocks, t, d), BF16), vmem((blocks, t, d), BF16),
            vmem((blocks, t, d), BF16), vmem((blocks, t, d), BF16),
            dma((5,)), *[dma((4, PIECES)) for _ in range(8)],
        ],
        compiler_params=pltpu.CompilerParams(
            collective_id=0, has_side_effects=True, vmem_limit_bytes=50 * 1024 * 1024
        ),
    )(*[pltpu.with_memory_space_constraint(x, pltpu.HBM) for x in (query, key_value, d_out, doc_starts.reshape(1, -1))])
    return pl.pallas_call(
        put_out,
        out_shape=tuple(jax.ShapeDtypeStruct(x.shape, BF16) for x in made),
        in_specs=[pl.BlockSpec(memory_space=pl.ANY)] * 2,
        out_specs=(hbm, hbm),
        scratch_shapes=[dma((2, 2))],
        compiler_params=pltpu.CompilerParams(vmem_limit_bytes=1024 * 1024),
    )(*made)


def put_out(dq, dkv, dq_hbm, dkv_hbm, sem):
    half = dq.shape[0] // 2
    copies = [
        pltpu.make_async_copy(
            source.at[pl.ds(part * half, half)], target.at[pl.ds(part * half, half)], sem.at[i, part]
        )
        for i, (source, target) in enumerate(((dq, dq_hbm), (dkv, dkv_hbm)))
        for part in range(2)
    ]
    for copy in copies:
        copy.start()
    for copy in copies:
        copy.wait()


def solution(mesh):
    placed = (P("ctx", "head"), P("ctx", "head"), P("ctx", "head"), P("head"))
    return jax.shard_map(
        functools.partial(shards, mesh.shape["ctx"]),
        mesh=mesh,
        in_specs=placed,
        out_specs=(P("ctx", "head"), P("ctx", "head")),
        check_vma=False,
    )
```

```python
import functools

import jax
import jax.numpy as jnp
from jax import lax
from jax.experimental import pallas as pl
from jax.experimental.pallas import tpu as pltpu
from jax.sharding import PartitionSpec as P

MESH = pl.DeviceIdType.MESH
HOPS = 3
CHUNK = 256
PIECES = 3
COLUMN = 16
NEG = -1e30
F32 = jnp.float32
BF16 = jnp.bfloat16


def dot(a, b):
    return lax.dot_general(a, b, (((1,), (0,)), ((), ())), preferred_element_type=F32)


def dot_t(a, b):
    return lax.dot_general(a, b, (((1,), (1,)), ((), ())), preferred_element_type=F32)


def kernel(
    n, q_hbm, kv_hbm, g_hbm, starts_hbm, dq_out, dkv_out,
    starts, qv, gv, kb, vb, qt, gt, kt, bias, docs, eb, gp, sbuf, mrun, trun, mblk, dblk, scl, dlt, dqt,
    own_v, own_k, shv, shk, rbv, rbk,
    load_sem, sk, sv, rk, rv, sent_v, sent_k, got_v, got_k,
):
    me = lax.axis_index("ctx")
    row = lax.axis_index("head")
    odd = lax.rem(me, 2)
    even = odd == 0
    t, d = kb.shape[1], kb.shape[2]
    heads = qt.shape[0]
    chunks = t // CHUNK
    unit = d ** (-0.5)
    to_exp2 = unit * 1.4426950408889634

    def dev(step):
        return (lax.rem(me + step + n, n), row)

    loads = [
        pltpu.make_async_copy(kv_hbm.at[:, pl.ds(0, d)], kb.at[0], load_sem.at[0]),
        pltpu.make_async_copy(q_hbm, qv, load_sem.at[1]),
        pltpu.make_async_copy(kv_hbm.at[:, pl.ds(d, d)], vb.at[0], load_sem.at[2]),
        pltpu.make_async_copy(g_hbm, gv, load_sem.at[3]),
        pltpu.make_async_copy(starts_hbm, starts, load_sem.at[4]),
    ]
    for load in loads:
        load.start()

    barrier = pltpu.get_barrier_semaphore()

    first_chip = lax.rem(me, COLUMN) < 2
    second_even = lax.rem(me, COLUMN) == 2
    late = lax.rem(me, COLUMN) == 6
    has_prev = me >= 2
    has_next = me < n - 2

    def greet(partner, senders, receivers):
        def hail(step):
            pl.semaphore_signal(barrier, inc=1, device_id=dev(step), device_id_type=MESH)

        hail(partner[0])

        @pl.when(has_prev)
        def _():
            for step in senders:
                hail(step)

        pl.semaphore_wait(barrier, jnp.where(has_next, 1 + len(receivers), 1))

    @pl.when(even)
    def _():
        greet((1,), (-1, -2), (3, 2))

    @pl.when(odd == 1)
    def _():
        greet((-1,), (-3,), (1,))

    piece = t // PIECES
    keys = (kb, sk, rk)
    values = (vb, sv, rv)

    def forward(group, which, source, slot, step, r):
        buf, send, recv = group
        rows = pl.ds(r * piece, piece)
        return pltpu.make_async_remote_copy(
            src_ref=buf.at[source, rows], dst_ref=buf.at[slot, rows],
            send_sem=send.at[which, r], recv_sem=recv.at[slot, r],
            device_id=dev(step), device_id_type=MESH,
        )

    def to_link(group, r):
        return forward(group, 0, 0, 3 - 2 * odd, 3 - 2 * odd, r)

    def to_partner(group, r):
        return forward(group, 1, 0, 1, 1, r)

    def relay_partner(group, r):
        return forward(group, 2, 1 + 2 * odd, 2, 1 - 2 * odd, r)

    def relay_link(group, r):
        return forward(group, 3, 1, 3, 2, r)

    def await_piece(group, slot, r):
        forward(group, 0, 0, slot, 1, r).wait_recv()

    def await_block(group, slot):
        for r in range(PIECES):
            await_piece(group, slot, r)

    def send_own_link(group):
        @pl.when(has_next)
        def _():
            for r in range(PIECES):
                to_link(group, r).start()

    def send_own_partner(group):
        for r in range(PIECES):
            to_partner(group, r).start()

    def pass_on_even(group, r):
        @pl.when(has_prev)
        def _():
            await_piece(group, 1, r)

            @pl.when(has_next)
            def _():
                relay_link(group, r).start()

            relay_partner(group, r).start()

    def pass_on_odd(group, r):
        @pl.when(has_prev)
        def _():
            await_piece(group, 3, r)
            relay_partner(group, r).start()

    loads[0].wait()
    send_own_link(keys)

    @pl.when(even)
    def _():
        send_own_partner(keys)

    loads[2].wait()

    @pl.when(first_chip)
    def _():
        send_own_link(values)

        @pl.when(even)
        def _():
            send_own_partner(values)

    loads[1].wait()
    loads[4].wait()
    for h in range(heads):
        qt[h] = qv[:, h * d:(h + 1) * d].T
    kt[0] = kb[0].T

    for b in range(1, HOPS + 1):
        @pl.when(me < b)
        def _():
            kb[b] = jnp.zeros((t, d), BF16)
            vb[b] = jnp.zeros((t, d), BF16)

    count = starts.shape[1]
    first = jnp.broadcast_to(starts[...].astype(F32), (count, count))
    lane = lax.broadcasted_iota(jnp.int32, (count, count), 1)
    after = jnp.where(lane == count - 1, float(n * t), pltpu.roll(first, count - 1, 1))
    first_q, after_q = first.T[:, :1], after.T[:, :1]
    at = (me * t + lax.broadcasted_iota(jnp.int32, (count, t), 1)).astype(F32)
    bias[...] = jnp.where((at >= first_q) & (at < after_q), 0.0, NEG).astype(BF16)

    def mark_docs(b):
        j = ((me - b) * t + lax.broadcasted_iota(jnp.int32, (t, count), 0)).astype(F32)
        inside = (j >= first[:1]) & (j < after[:1])
        docs[b] = jnp.where(inside | (j < 0.0), 1.0, 0.0).astype(BF16)

    for b in range(HOPS + 1):
        mark_docs(b)

    def scores(b, own):
        for h in range(heads):
            for c in range(chunks):
                lanes = slice(c * CHUNK, (c + 1) * CHUNK)
                rows = (c + 1) * CHUNK if own else t
                slot = (h * chunks + c) % 2
                left = jnp.concatenate([kb[b, :rows, :], docs[b, :rows, :]], axis=1)
                right = jnp.concatenate([qt[h, :, lanes], bias[:, lanes]], axis=0)
                s = dot(left, right) * to_exp2
                if own:
                    j = lax.broadcasted_iota(jnp.int32, (rows, CHUNK), 0)
                    p = lax.broadcasted_iota(jnp.int32, (rows, CHUNK), 1) + c * CHUNK
                    s = jnp.where(j <= p, s, NEG)
                sbuf[slot, :rows, :] = s
                top = jnp.max(s, axis=0, keepdims=True)
                if not own:
                    before = mrun[h:h + 1, lanes]
                    top = jnp.maximum(before, top)
                e = jnp.exp2(sbuf[slot, :rows, :] - top)
                total = jnp.sum(e, axis=0, keepdims=True)
                if not own:
                    total = total + trun[h:h + 1, lanes] * jnp.exp2(before - top)
                eb[b, h, :rows, lanes] = e.astype(BF16)
                if rows < t:
                    eb[b, h, rows:, lanes] = jnp.zeros((t - rows, CHUNK), BF16)
                mrun[h:h + 1, lanes] = top
                mblk[b, h:h + 1, lanes] = top
                trun[h:h + 1, lanes] = total

    def grad_probs(b, own):
        for h in range(heads):
            for c in range(chunks):
                lanes = slice(c * CHUNK, (c + 1) * CHUNK)
                rows = (c + 1) * CHUNK if own else t
                x = dot(vb[b, :rows, :], gt[h, :, lanes])
                gp[b, h, :rows, lanes] = x
                dblk[b, h:h + 1, lanes] = jnp.sum(
                    eb[b, h, :rows, lanes].astype(F32) * x, axis=0, keepdims=True
                )

    def grad_probs_piece(b, r):
        rows = slice(r * piece, (r + 1) * piece)
        for h in range(heads):
            for c in range(chunks):
                lanes = slice(c * CHUNK, (c + 1) * CHUNK)
                x = dot(vb[b, rows, :], gt[h, :, lanes])
                gp[b, h, rows, lanes] = x
                part = jnp.sum(eb[b, h, rows, lanes].astype(F32) * x, axis=0, keepdims=True)
                dblk[b, h:h + 1, lanes] = part if r == 0 else dblk[b, h:h + 1, lanes] + part

    def grad_scores(b, own):
        for h in range(heads):
            for c in range(chunks):
                lanes = slice(c * CHUNK, (c + 1) * CHUNK)
                rows = (c + 1) * CHUNK if own else t
                eb[b, h, :rows, lanes] = (
                    eb[b, h, :rows, lanes].astype(F32) * (gp[b, h, :rows, lanes] - dlt[h:h + 1, lanes])
                ).astype(BF16)

    def contract(b, rights, factor):
        total = None
        for h in range(heads):
            right = (rights[h].astype(F32) * (scl[b, h:h + 1, :] * factor)).astype(BF16)
            term = dot_t(eb[b, h], right)
            total = term if total is None else total + term
        return total

    def grad_query(b, first):
        for h in range(heads):
            for c in range(chunks):
                lanes = slice(c * CHUNK, (c + 1) * CHUNK)
                x = dot(kt[b], eb[b, h, :, lanes]) * (scl[b, h:h + 1, lanes] * unit)
                dqt[h, :, lanes] = x if first else dqt[h, :, lanes] + x

    scores(0, True)
    loads[3].wait()
    for h in range(heads):
        gt[h] = gv[:, h * d:(h + 1) * d].T
    grad_probs(0, True)

    def arrive(step):
        return jnp.where(jnp.logical_and(odd == 1, step > 1), 5 - step, step)

    def k_step(step, carry):
        b = arrive(step)

        @pl.when(jnp.logical_and(even, step == 1))
        def _():
            for r in range(PIECES):
                pass_on_even(keys, r)

            @pl.when(jnp.logical_not(first_chip))
            def _():
                send_own_link(values)
                send_own_partner(values)

        @pl.when(jnp.logical_and(odd == 1, step == 2))
        def _():
            for r in range(PIECES):
                pass_on_odd(keys, r)

            @pl.when(jnp.logical_not(first_chip))
            def _():
                send_own_link(values)

        @pl.when(jnp.logical_and(second_even, step == HOPS))
        def _():
            for r in range(PIECES):
                pass_on_even(values, r)

        @pl.when(jnp.logical_and(step != 1 + odd, me >= b))
        def _():
            await_block(keys, b)

        scores(b, False)
        kt[b] = kb[b].T
        return carry

    lax.fori_loop(1, HOPS + 1, k_step, 0)

    usual_even = jnp.logical_and(even, jnp.logical_not(second_even))

    @pl.when(usual_even)
    def _():
        pass_on_even(values, 0)

    for h in range(heads):
        inverse = 1.0 / trun[h:h + 1, :]
        for b in range(HOPS + 1):
            scl[b, h:h + 1, :] = jnp.exp2(mblk[b, h:h + 1, :] - mrun[h:h + 1, :]) * inverse

    def off_of(step):
        on_odd = jnp.where(step == 2, 3, 2 - step)
        return jnp.where(even, 3 - step, on_odd)

    sides = {"v": (shv, rbv, sent_v, got_v), "k": (shk, rbk, sent_k, got_k)}

    def back(side, off, r):
        send_buf, land, send, recv = sides[side]
        step = jnp.where(even, jnp.where(off == 1, -1, jnp.where(off == 2, 1, -2)), jnp.where(off == 3, -3, -1))
        slot = jnp.where(off == 1, 2, jnp.where(off == 2, 0, jnp.where(even, 1, 3)))
        rows = pl.ds(r * piece, piece)
        return pltpu.make_async_remote_copy(
            src_ref=send_buf.at[off, rows], dst_ref=land.at[slot, rows],
            send_sem=send.at[off, r], recv_sem=recv.at[slot, r],
            device_id=dev(step), device_id_type=MESH,
        )

    def send_back(side, off):
        for r in range(PIECES):
            back(side, off, r).start()

    def landed(side, slot, r):
        send_buf, land, send, recv = sides[side]
        rows = pl.ds(r * piece, piece)
        pltpu.make_async_remote_copy(
            src_ref=land.at[slot, rows], dst_ref=land.at[slot, rows],
            send_sem=send.at[0, r], recv_sem=recv.at[slot, r],
            device_id=dev(1), device_id_type=MESH,
        ).wait_recv()

    def share_step(side, rights, factor, extra):
        def run(step, carry):
            off = off_of(step)
            if side == "k":
                grad_scores(off, False)
            sides[side][0][off] = contract(off, rights, factor).astype(BF16)

            @pl.when(jnp.logical_and(step < 2, me >= off))
            def _():
                send_back(side, off)

            if extra is not None:
                extra(step)

            return carry

        lax.fori_loop(0, HOPS, run, 0)

    def add_landed(side, off, slot, r):
        send_buf, land, send, recv = sides[side]
        rows = slice(r * piece, (r + 1) * piece)
        landed(side, slot, r)
        total = send_buf[off, rows].astype(F32) + land[slot, rows].astype(F32)
        send_buf[off, rows] = total.astype(BF16)

    def combine_odd(side, r):
        @pl.when(has_prev)
        def _():
            add_landed(side, 3, 0, r)
            back(side, 3, r).start()

    def combine_even(side, r):
        send_buf, land, send, recv = sides[side]
        rows = slice(r * piece, (r + 1) * piece)

        @pl.when(jnp.logical_and(has_prev, has_next))
        def _():
            landed(side, 0, r)
            landed(side, 1, r)
            total = send_buf[1, rows].astype(F32) + land[0, rows].astype(F32)
            send_buf[1, rows] = (total + land[1, rows].astype(F32)).astype(BF16)

        @pl.when(jnp.logical_and(has_prev, jnp.logical_not(has_next)))
        def _():
            add_landed(side, 1, 0, r)

        @pl.when(has_prev)
        def _():
            back(side, 1, r).start()

    def relay_second(step):
        @pl.when(jnp.logical_and(usual_even, step == 1))
        def _():
            pass_on_even(values, 1)

    share_step("v", gt, 1.0, relay_second)
    own_v[...] = contract(0, gt, 1.0)

    def v_step(step, carry):
        b = arrive(step)

        @pl.when(jnp.logical_and(usual_even, step == 1))
        def _():
            pass_on_even(values, 2)

        @pl.when(jnp.logical_and(odd == 1, step == 2))
        def _():
            pass_on_odd(values, 0)
            pass_on_odd(values, 1)
            for r in range(PIECES):
                combine_odd("v", r)
            pass_on_odd(values, 2)

        @pl.when(jnp.logical_and(jnp.logical_and(even, jnp.logical_not(late)), step == 3))
        def _():
            for r in range(PIECES):
                combine_even("v", r)

        for r in range(PIECES):
            @pl.when(jnp.logical_and(step != 1 + odd, me >= b))
            def _():
                await_piece(values, b, r)

            grad_probs_piece(b, r)

        return carry

    lax.fori_loop(1, HOPS + 1, v_step, 0)

    for h in range(heads):
        delta = None
        for b in range(HOPS + 1):
            term = dblk[b, h:h + 1, :] * scl[b, h:h + 1, :]
            delta = term if delta is None else delta + term
        dlt[h:h + 1, :] = delta

    share_step("k", qt, unit, None)

    @pl.when(jnp.logical_and(even, late))
    def _():
        for r in range(PIECES):
            combine_even("v", r)

    @pl.when(odd == 1)
    def _():
        for r in range(PIECES):
            combine_odd("k", r)


    grad_query(3, True)
    for r in range(PIECES):
        @pl.when(even)
        def _():
            combine_even("k", r)

        if r == 0:
            grad_query(2, False)
        if r == 1:
            grad_query(1, False)
        if r == 2:
            grad_scores(0, True)
            own_k[...] = contract(0, qt, unit)
            grad_query(0, False)

    for h in range(heads):
        dq_out[:, h * d:(h + 1) * d] = dqt[h].T.astype(BF16)

    for side, own, column in (("v", own_v, d), ("k", own_k, 0)):
        land = sides[side][1]

        @pl.when(jnp.logical_or(even, has_next))
        def _():
            for r in range(PIECES):
                landed(side, 2, r)
            own[...] = own[...] + land[2].astype(F32)

        @pl.when(jnp.logical_and(even, has_next))
        def _():
            for r in range(PIECES):
                landed(side, 3, r)
            own[...] = own[...] + land[3].astype(F32)

        dkv_out[:, column:column + d] = own[...].astype(BF16)

    for r in range(PIECES):
        for group in (keys, values):
            @pl.when(has_next)
            def _():
                to_link(group, r).wait_send()

            @pl.when(has_prev)
            def _():
                relay_partner(group, r).wait_send()

            @pl.when(even)
            def _():
                to_partner(group, r).wait_send()

            @pl.when(jnp.logical_and(even, jnp.logical_and(has_prev, has_next)))
            def _():
                relay_link(group, r).wait_send()

        for side in ("v", "k"):
            for off in range(1, HOPS + 1):
                @pl.when(me >= off)
                def _():
                    back(side, off, r).wait_send()


def shards(n, query, key_value, d_out, doc_starts):
    t, width = key_value.shape
    d = width // 2
    heads = query.shape[1] // d
    blocks = HOPS + 1
    hbm = pl.BlockSpec(memory_space=pltpu.HBM)
    vmem = pltpu.VMEM
    dma = pltpu.SemaphoreType.DMA
    made = pl.pallas_call(
        functools.partial(kernel, n),
        out_shape=(
            jax.ShapeDtypeStruct(query.shape, BF16),
            jax.ShapeDtypeStruct(key_value.shape, BF16),
        ),
        in_specs=[hbm, hbm, hbm, hbm],
        out_specs=(pl.BlockSpec(memory_space=vmem), pl.BlockSpec(memory_space=vmem)),
        scratch_shapes=[
            vmem((1, doc_starts.shape[0]), jnp.int32),
            vmem((t, heads * d), BF16), vmem((t, heads * d), BF16),
            vmem((blocks, t, d), BF16), vmem((blocks, t, d), BF16),
            vmem((heads, d, t), BF16), vmem((heads, d, t), BF16), vmem((blocks, d, t), BF16),
            vmem((doc_starts.shape[0], t), BF16), vmem((blocks, t, doc_starts.shape[0]), BF16),
            vmem((blocks, heads, t, t), BF16), vmem((blocks, heads, t, t), F32),
            vmem((2, t, CHUNK), F32),
            vmem((heads, t), F32), vmem((heads, t), F32),
            vmem((blocks, heads, t), F32), vmem((blocks, heads, t), F32), vmem((blocks, heads, t), F32),
            vmem((heads, t), F32), vmem((heads, d, t), F32),
            vmem((t, d), F32), vmem((t, d), F32),
            vmem((blocks, t, d), BF16), vmem((blocks, t, d), BF16),
            vmem((blocks, t, d), BF16), vmem((blocks, t, d), BF16),
            dma((5,)), *[dma((4, PIECES)) for _ in range(8)],
        ],
        compiler_params=pltpu.CompilerParams(
            collective_id=0, has_side_effects=True, vmem_limit_bytes=50 * 1024 * 1024
        ),
    )(*[pltpu.with_memory_space_constraint(x, pltpu.HBM) for x in (query, key_value, d_out, doc_starts.reshape(1, -1))])
    return pl.pallas_call(
        put_out,
        out_shape=tuple(jax.ShapeDtypeStruct(x.shape, BF16) for x in made),
        in_specs=[pl.BlockSpec(memory_space=pl.ANY)] * 2,
        out_specs=(hbm, hbm),
        scratch_shapes=[dma((2, 2))],
        compiler_params=pltpu.CompilerParams(vmem_limit_bytes=1024 * 1024),
    )(*made)


def put_out(dq, dkv, dq_hbm, dkv_hbm, sem):
    half = dq.shape[0] // 2
    copies = [
        pltpu.make_async_copy(
            source.at[pl.ds(part * half, half)], target.at[pl.ds(part * half, half)], sem.at[i, part]
        )
        for i, (source, target) in enumerate(((dq, dq_hbm), (dkv, dkv_hbm)))
        for part in range(2)
    ]
    for copy in copies:
        copy.start()
    for copy in copies:
        copy.wait()


def solution(mesh):
    placed = (P("ctx", "head"), P("ctx", "head"), P("ctx", "head"), P("head"))
    return jax.shard_map(
        functools.partial(shards, mesh.shape["ctx"]),
        mesh=mesh,
        in_specs=placed,
        out_specs=(P("ctx", "head"), P("ctx", "head")),
        check_vma=False,
    )
```
